32 devices in a mesh: grp: 4 (over y, x), dev: 8 (over z, core).
Axes of the slice: x: 2, y: 2, z: 4, core: 2. Of those that a mesh axis runs over, the one named last changes fastest.
Arguments:
- acts: bfloat16 [8192, 12288], P(('grp', 'dev')), may hold values from -6 to 6
- grads_out: bfloat16 [8192, 64], P(('grp', 'dev')), may hold values from -0.375 to 0.375
- residual_in: float32 [32, 64, 12288], P(('grp', 'dev')), may hold values from -6 to 6
- sel_index: int32 [32, 64], P(('grp', 'dev')), may hold values from 0 to 6143, as said below
- sel_count: int32 [32], P(('grp', 'dev')), may hold values from 16 to 64, as said below
- momentum_in: float32 [64, 12288], P(None, 'dev'), may hold values from -6 to 6
Outputs:
- residual_out: float32 [32, 64, 12288], P(('grp', 'dev'))
- momentum_out: float32 [64, 12288], P(None, 'dev')
The draws below stay inside these ranges and needn't reach their ends.
Inputs may be any that keep to these rules, and one draw needn't show every extreme that they name: `sel_index`: the 64 numbers of a row are distinct. `sel_count`: equal to 64 on some device in every draw.
All inputs are finite; a program needn't handle non-finite values.
Results may differ from the reference program's by a relative error of at most 0.0003.
Values sent between devices are 32-bit elements; how exact they have to be, the bound alone decides.
A program may use at most 64 MiB of HBM per device.

```python
import jax
import jax.numpy as jnp
from jax import lax

D = 12288
COLS = 64
TOK_DEV = 256
KSEL = 64
NBLK = 6144
TOKENS = 8192
DEVICES = 32


def draw_sel_index(key, part):
    keys = jax.random.split(jax.random.fold_in(key, 11), DEVICES)

    def one_row(row_key):
        return jax.random.permutation(row_key, NBLK)[:KSEL]
    return jax.vmap(one_row)(keys).astype(jnp.int32)


def draw_sel_count(key, part):
    counts = jax.random.randint(jax.random.fold_in(key, 23), (DEVICES,), KSEL // 4, KSEL + 1)
    fullest = jax.random.randint(jax.random.fold_in(key, 29), (), 0, DEVICES)
    return counts.at[fullest].set(KSEL).astype(jnp.int32)


def shard_levels(key, dims, pieces, least, largest):
    def one(axis_at, shards_of):
        steps = jax.random.uniform(jax.random.fold_in(jax.random.fold_in(key, 6), axis_at), (shards_of,), jnp.float32, least / len(pieces), largest / len(pieces))
        return jnp.repeat(jnp.exp(steps), dims[axis_at] // shards_of).reshape((-1,) + (1,) * (len(dims) - axis_at - 1))

    gain = one(*pieces[0])
    for cut in pieces[1:]:
        gain = gain * one(*cut)
    return gain


def centred(stream_key, dims, scale, limit, cuts=(), held_as=jnp.bfloat16):
    result = scale * jax.random.normal(stream_key, dims, jnp.float32)
    if cuts:
        result = result * shard_levels(stream_key, dims, cuts, -0.22, 0.18)
    return jnp.clip(result, -limit, limit).astype(held_as)


def setup_inputs(seed: int = 0) -> dict:
    splits = jax.random.split(jax.random.key(seed), 7)
    acts = centred(splits[0], (TOKENS, D), 1.0, 6.0, ((0, 32),))
    grads_out = centred(splits[1], (TOKENS, COLS), TOK_DEV ** -0.5, 0.375, ((0, 32),))
    residual_in = centred(splits[2], (DEVICES, COLS, D), 1.0, 6.0, ((0, 32),), jnp.float32)
    sel_index = draw_sel_index(jax.random.fold_in(splits[6], 71), 0)
    sel_count = draw_sel_count(jax.random.fold_in(splits[6], 71), 0)
    momentum_in = centred(splits[5], (COLS, D), 1.0, 6.0, ((1, 8),), jnp.float32)
    return {"acts": acts, "grads_out": grads_out, "residual_in": residual_in, "sel_index": sel_index, "sel_count": sel_count, "momentum_in": momentum_in}


def one_device(operands):
    inputs, out_grads, residual, chosen, how_many = operands
    local_grad = lax.dot_general(out_grads, inputs, (((0,), (0,)), ((), ())), preferred_element_type=jnp.float32)
    summed = residual + local_grad
    blocks = summed.reshape(NBLK, 128)
    valid_rows = (jnp.arange(KSEL, dtype=jnp.int32) < how_many).astype(jnp.float32)
    picked = blocks[chosen] * valid_rows[:, None]
    marked = jnp.zeros((NBLK,), jnp.float32).at[chosen].max(valid_rows)
    kept = blocks * (1.0 - marked)[:, None]
    return kept.reshape(COLS, D), picked


def reference(acts, grads_out, residual_in, sel_index, sel_count, momentum_in):
    inputs = acts.reshape(DEVICES, TOK_DEV, D)
    out_grads = grads_out.reshape(DEVICES, TOK_DEV, COLS)
    residual_out, picked = lax.map(one_device, (inputs, out_grads, residual_in, sel_index, sel_count))
    spread = jnp.zeros((NBLK, 128), jnp.float32).at[sel_index.reshape(-1)].add(picked.reshape(-1, 128))
    momentum_out = 0.9 * momentum_in + spread.reshape(COLS, D)
    return residual_out, momentum_out
```

```python
import functools

import jax
import jax.numpy as jnp
from jax import lax
from jax.experimental import pallas as pl
from jax.experimental.pallas import tpu as pltpu
from jax.sharding import PartitionSpec as P

momentum_decay = 0.9
LANES = 128
MESH = pl.DeviceIdType.MESH


def tiles_of(width):
    for count in (8, 6, 4, 3, 2):
        if width % (count * 2 * LANES) == 0:
            return count
    return 1


def local_kernel(
    tiles, acts, residual, grads, sel_row, sel_smem, count_smem,
    kept, packed,
    acts_buf, res_buf, summed, kept_buf, in_sem, out_sem,
):
    columns, width = residual.shape[1:]
    slots = sel_row.shape[1]
    blocks_wide = width // LANES
    span = width // tiles
    per_tile = span // LANES

    def fetch(t):
        cols = pl.ds(t * span, span)
        return (
            pltpu.make_async_copy(acts.at[:, cols], acts_buf.at[:, cols], in_sem.at[0, t]),
            pltpu.make_async_copy(residual.at[0, :, cols], res_buf.at[:, cols], in_sem.at[1, t]),
        )

    def put(t):
        cols = pl.ds(t * span, span)
        return pltpu.make_async_copy(kept_buf.at[:, cols], kept.at[0, :, cols], out_sem.at[t])

    for t in range(tiles):
        for copy in fetch(t):
            copy.start()

    number = sel_row[...].astype(jnp.float32)
    row = jnp.floor((number + 0.5) * (1.0 / blocks_wide))
    col = number - row * blocks_wide
    used = lax.broadcasted_iota(jnp.int32, (1, slots), 1) < count_smem[0]
    row_hit = lax.broadcasted_iota(jnp.int32, (columns, slots), 0).astype(jnp.float32) == row
    col_hit = lax.broadcasted_iota(jnp.int32, (blocks_wide, slots), 0).astype(jnp.float32) == col
    taken = lax.dot_general(
        jnp.where(row_hit & used, 1.0, 0.0).astype(jnp.bfloat16),
        jnp.where(col_hit, 1.0, 0.0).astype(jnp.bfloat16),
        (((1,), (1,)), ((), ())),
        preferred_element_type=jnp.float32,
    )
    label = jnp.where(used, col * columns + row, -1.0)
    packed[pl.ds(slots, 8), pl.ds(0, slots)] = jnp.broadcast_to(label, (8, slots))
    if slots < LANES:
        packed[pl.ds(slots, 8), pl.ds(slots, LANES - slots)] = jnp.full(
            (8, LANES - slots), -1.0, jnp.float32
        )

    turned = grads[...].T
    for t in range(tiles):
        for copy in fetch(t):
            copy.wait()
        cols = pl.ds(t * span, span)
        total = res_buf[:, cols] + jnp.dot(
            turned, acts_buf[:, cols], preferred_element_type=jnp.float32
        )
        for j in range(per_tile):
            c = t * per_tile + j
            piece = total[:, j * LANES : (j + 1) * LANES]
            summed[c] = piece
            kept_buf[:, pl.ds(c * LANES, LANES)] = jnp.where(taken[:, c : c + 1] > 0.5, 0.0, piece)
        put(t).start()

    for s in range(slots):
        b = sel_smem[0, s]
        r = lax.div(b, blocks_wide)
        c = b - r * blocks_wide
        packed[pl.ds(s, 1), :] = summed[c, pl.ds(r, 1), :]

    for t in range(tiles):
        put(t).wait()


def gather_kernel(
    sizes, packed, momentum_in, momentum_out, store, total, send_sem, recv_sem
):
    rows_a, rows_b, depth, cores = sizes
    slots = packed.shape[0] - 8
    columns, part_width = momentum_in.shape
    part_blocks = part_width // LANES
    g = lax.axis_index("grp")
    d = lax.axis_index("dev")
    a, b = g // rows_b, g % rows_b
    z, core = d // cores, d % cores

    def group(i, j):
        return lax.rem(a + i, rows_a) * rows_b + lax.rem(b + j, rows_b)

    def member(k, q):
        return lax.rem(z + k, depth) * cores + lax.rem(core + q, cores)

    peers = (
        [(g, member(k, 0)) for k in range(1, depth)]
        + [(g, member(0, q)) for q in range(1, cores)]
        + [(group(i, 0), d) for i in range(1, rows_a)]
        + [(group(0, j), d) for j in range(1, rows_b)]
    )
    barrier = pltpu.get_barrier_semaphore()
    for peer in peers:
        pl.semaphore_signal(barrier, inc=1, device_id=peer, device_id_type=MESH)
    store[g, d] = packed[...]
    pl.semaphore_wait(barrier, len(peers))

    sends = []

    def copy_to(source, slot, peer, index):
        return pltpu.make_async_remote_copy(
            src_ref=source,
            dst_ref=store.at[slot[0], slot[1]],
            send_sem=send_sem.at[index],
            recv_sem=recv_sem.at[slot[0], slot[1]],
            device_id=peer,
            device_id_type=MESH,
        )

    def send(slot, peer, own=False):
        source = packed if own else store.at[slot[0], slot[1]]
        copy = copy_to(source, slot, peer, len(sends))
        sends.append(copy)
        copy.start()

    def arrived(slot):
        copy_to(store.at[slot[0], slot[1]], slot, (g, member(0, 1)), 0).wait_recv()

    def to_partner(slot, own=False):
        for q in range(1, cores):
            send(slot, (g, member(0, q)), own)

    def spread(k, own=False):
        slot = (g, member(k, 0))
        for i in range(1, rows_a):
            send(slot, (group(i, 0), d), own)
        for j in range(1, rows_b):
            send(slot, (group(0, j), d), own)
        to_partner(slot, own)

    base = (d * (part_blocks * columns)).astype(jnp.float32)
    place = lax.broadcasted_iota(jnp.int32, (part_blocks * columns, 1), 0).astype(jnp.float32)
    started = []

    def add(i, j, q):
        blocks = [(group(i, j), member(k, q)) for k in range(depth)]
        vals = jnp.concatenate([store[x, y, :slots, :] for x, y in blocks], axis=0)
        labels = jnp.concatenate(
            [store[x, y, pl.ds(slots, 1), pl.ds(0, slots)] for x, y in blocks], axis=1
        )
        high = vals.astype(jnp.bfloat16)
        low = (vals - high.astype(jnp.float32)).astype(jnp.bfloat16)
        both = jnp.concatenate([high, low], axis=1)
        hit = jnp.where(place == labels - base, 1.0, 0.0).astype(jnp.bfloat16)
        part = jnp.dot(hit, both, preferred_element_type=jnp.float32)
        if started:
            total[...] += part
        else:
            total[...] = part
            started.append(True)

    def add_others(i, j):
        for q in range(1, cores):
            for k in range(depth):
                arrived((group(i, j), member(k, q)))
            add(i, j, q)

    for k in range(1, depth):
        send((g, d), (g, member(depth - k, 0)), True)
    spread(0, True)
    order = sorted(range(1, depth), key=lambda k: min(k, depth - k))
    hops = [(k, i, j) for k in range(depth) for i, j in (
        [(0, j) for j in range(1, rows_b)] if k % 2 == 0 else [(i, 0) for i in range(1, rows_a)]
    )]

    def relay(k, i, j):
        slot = (group(i, j), member(k, 0))
        arrived(slot)
        if j:
            for n in range(1, rows_a):
                send(slot, (group(n, 0), d))
        else:
            for n in range(1, rows_b):
                send(slot, (group(0, n), d))
        to_partner(slot)

    for k in order:
        arrived((g, member(k, 0)))
        spread(k)
    for k, i, j in hops:
        if k == 0:
            relay(k, i, j)
    add(0, 0, 0)
    for k, i, j in hops:
        if k:
            relay(k, i, j)
    add_others(0, 0)
    for i in range(rows_a):
        for j in range(rows_b):
            if i == 0 and j == 0:
                continue
            for k in range(depth):
                relayed = (k, i, j) in hops
                if not relayed:
                    slot = (group(i, j), member(k, 0))
                    arrived(slot)
                    to_partner(slot)
            add(i, j, 0)
            if (i, j) != (rows_a - 1, rows_b - 1) or True:
                add_others(i, j)

    for c in range(part_blocks):
        rows = pl.ds(c * columns, columns)
        cols = pl.ds(c * LANES, LANES)
        momentum_out[:, cols] = momentum_decay * momentum_in[:, cols] + (
            total[rows, pl.ds(0, LANES)] + total[rows, pl.ds(LANES, LANES)]
        )
    for copy in sends:
        copy.wait_send()


def local(mesh_sizes, acts, grads_out, residual_in, sel_index, sel_count, momentum_in):
    groups, members = mesh_sizes
    tokens, width = acts.shape
    columns = grads_out.shape[1]
    slots = sel_index.shape[1]
    part_width = momentum_in.shape[1]
    tiles = tiles_of(width)
    vmem = pl.BlockSpec(memory_space=pltpu.VMEM)
    smem = pl.BlockSpec(memory_space=pltpu.SMEM)
    hbm = pl.BlockSpec(memory_space=pl.ANY)
    kept, packed = pl.pallas_call(
        functools.partial(local_kernel, tiles),
        out_shape=(
            jax.ShapeDtypeStruct(residual_in.shape, jnp.float32),
            jax.ShapeDtypeStruct((slots + 8, LANES), jnp.float32),
        ),
        in_specs=[hbm, hbm, vmem, vmem, smem, smem],
        out_specs=(hbm, vmem),
        scratch_shapes=[
            pltpu.VMEM((tokens, width), jnp.bfloat16),
            pltpu.VMEM((columns, width), jnp.float32),
            pltpu.VMEM((width // LANES, columns, LANES), jnp.float32),
            pltpu.VMEM((columns, width), jnp.float32),
            pltpu.SemaphoreType.DMA((2, tiles)),
            pltpu.SemaphoreType.DMA((tiles,)),
        ],
        name="select",
    )(acts, residual_in, grads_out, sel_index, sel_index, sel_count)

    rows_b = max(n for n in range(1, groups + 1) if groups % n == 0 and n * n <= groups)
    cores = 2 if members % 2 == 0 else 1
    sizes = (groups // rows_b, rows_b, members // cores, cores)
    rows_a, rows_b, depth, cores = sizes
    n_sends = (
        depth - 1 + depth * (rows_a * rows_b - 1) + depth * groups * (cores - 1)
    )
    momentum_out = pl.pallas_call(
        functools.partial(gather_kernel, sizes),
        out_shape=jax.ShapeDtypeStruct(momentum_in.shape, jnp.float32),
        in_specs=[vmem, vmem],
        out_specs=vmem,
        scratch_shapes=[
            pltpu.VMEM((groups, members, slots + 8, LANES), jnp.float32),
            pltpu.VMEM((columns * part_width // LANES, 2 * LANES), jnp.float32),
            pltpu.SemaphoreType.DMA((n_sends,)),
            pltpu.SemaphoreType.DMA((groups, members)),
        ],
        compiler_params=pltpu.CompilerParams(collective_id=0, has_side_effects=True),
        name="gather",
    )(packed, momentum_in)
    return (kept, momentum_out)


def solution(mesh):
    placed = (
        P(("grp", "dev"), None),
        P(("grp", "dev"), None),
        P(("grp", "dev"), None, None),
        P(("grp", "dev"), None),
        P(("grp", "dev")),
        P(None, "dev"),
    )
    return jax.shard_map(
        functools.partial(local, (mesh.shape["grp"], mesh.shape["dev"])),
        mesh=mesh,
        in_specs=placed,
        out_specs=(P(("grp", "dev"), None, None), P(None, "dev")),
        check_vma=False,
    )
```

```python
import functools

import jax
import jax.numpy as jnp
from jax import lax
from jax.experimental import pallas as pl
from jax.experimental.pallas import tpu as pltpu
from jax.sharding import PartitionSpec as P

momentum_decay = 0.9
LANES = 128
MESH = pl.DeviceIdType.MESH


def tiles_of(width):
    for count in (8, 6, 4, 3, 2):
        if width % (count * 2 * LANES) == 0:
            return count
    return 1


def gather_kernel(
    tiles, sizes, acts, residual, grads_in, sel_in, sel_smem, count_smem, momentum_hbm,
    kept, momentum_out,
    grads, sel_row, momentum_in, small_sem, acts_buf, res_buf, summed, packed, store, total, in_sem, send_sem, recv_sem,
):
    columns, width = residual.shape[1:]
    slots = sel_row.shape[1]
    blocks_wide = width // LANES
    span = width // tiles
    per_tile = span // LANES

    def fetch(t):
        cols = pl.ds(t * span, span)
        return (
            pltpu.make_async_copy(acts.at[:, cols], acts_buf.at[:, cols], in_sem.at[0, t]),
            pltpu.make_async_copy(residual.at[0, :, cols], res_buf.at[:, cols], in_sem.at[1, t]),
        )

    small = [
        pltpu.make_async_copy(sel_in, sel_row, small_sem.at[0]),
        pltpu.make_async_copy(grads_in, grads, small_sem.at[1]),
        pltpu.make_async_copy(momentum_hbm, momentum_in, small_sem.at[2]),
    ]
    for copy in small[:2]:
        copy.start()
    for t in range(tiles):
        for copy in fetch(t):
            copy.start()
    small[2].start()

    rows_a, rows_b, depth, cores = sizes
    part_width = momentum_in.shape[1]
    part_blocks = part_width // LANES
    g = lax.axis_index("grp")
    d = lax.axis_index("dev")
    a, b = g // rows_b, g % rows_b
    z, core = d // cores, d % cores

    def group(i, j):
        return lax.rem(a + i, rows_a) * rows_b + lax.rem(b + j, rows_b)

    def member(k, q):
        return lax.rem(z + k, depth) * cores + lax.rem(core + q, cores)

    peers = (
        [(g, member(k, 0)) for k in range(1, depth)]
        + [(g, member(0, q)) for q in range(1, cores)]
        + [(group(i, 0), d) for i in range(1, rows_a)]
        + [(group(0, j), d) for j in range(1, rows_b)]
    )
    barrier = pltpu.get_barrier_semaphore()
    for peer in peers:
        pl.semaphore_signal(barrier, inc=1, device_id=peer, device_id_type=MESH)

    small[0].wait()
    number = sel_row[...].astype(jnp.float32)
    row = jnp.floor((number + 0.5) * (1.0 / blocks_wide))
    col = number - row * blocks_wide
    used = lax.broadcasted_iota(jnp.int32, (1, slots), 1) < count_smem[0]
    label = jnp.where(used, col * columns + row, -1.0)
    packed[pl.ds(slots, 8), pl.ds(0, slots)] = jnp.broadcast_to(label, (8, slots))
    if slots < LANES:
        packed[pl.ds(slots, 8), pl.ds(slots, LANES - slots)] = jnp.full(
            (8, LANES - slots), -1.0, jnp.float32
        )

    small[1].wait()
    turned = grads[...]
    for t in range(tiles):
        for copy in fetch(t):
            copy.wait()
        cols = pl.ds(t * span, span)
        sums = res_buf[:, cols] + jnp.dot(
            turned, acts_buf[:, cols], preferred_element_type=jnp.float32
        )
        for j in range(per_tile):
            summed[t * per_tile + j] = sums[:, j * LANES : (j + 1) * LANES]
    for s in range(slots):
        block = sel_smem[0, s]
        r = lax.div(block, blocks_wide)
        packed[pl.ds(s, 1), :] = summed[block - r * blocks_wide, pl.ds(r, 1), :]
    store[g, d] = packed[...]
    pl.semaphore_wait(barrier, len(peers))

    sends = []

    def copy_to(source, slot, peer, index):
        return pltpu.make_async_remote_copy(
            src_ref=source,
            dst_ref=store.at[slot[0], slot[1]],
            send_sem=send_sem.at[index],
            recv_sem=recv_sem.at[slot[0], slot[1]],
            device_id=peer,
            device_id_type=MESH,
        )

    def send(slot, peer, own=False):
        source = packed if own else store.at[slot[0], slot[1]]
        copy = copy_to(source, slot, peer, len(sends))
        sends.append(copy)
        copy.start()

    def arrived(slot):
        copy_to(store.at[slot[0], slot[1]], slot, (g, member(0, 1)), 0).wait_recv()

    def to_partner(slot, own=False):
        for q in range(1, cores):
            send(slot, (g, member(0, q)), own)

    def spread(k, own=False):
        slot = (g, member(k, 0))
        for i in range(1, rows_a):
            send(slot, (group(i, 0), d), own)
        for j in range(1, rows_b):
            send(slot, (group(0, j), d), own)
        to_partner(slot, own)

    base = (d * (part_blocks * columns)).astype(jnp.float32)
    place = lax.broadcasted_iota(jnp.int32, (part_blocks * columns, 1), 0).astype(jnp.float32)
    started = []

    def add(i, j, q):
        blocks = [(group(i, j), member(k, q)) for k in range(depth)]
        vals = jnp.concatenate([store[x, y, :slots, :] for x, y in blocks], axis=0)
        labels = jnp.concatenate(
            [store[x, y, pl.ds(slots, 1), pl.ds(0, slots)] for x, y in blocks], axis=1
        )
        high = vals.astype(jnp.bfloat16)
        low = (vals - high.astype(jnp.float32)).astype(jnp.bfloat16)
        both = jnp.concatenate([high, low], axis=1)
        hit = jnp.where(place == labels - base, 1.0, 0.0).astype(jnp.bfloat16)
        part = jnp.dot(hit, both, preferred_element_type=jnp.float32)
        if started:
            total[...] += part
        else:
            total[...] = part
            started.append(True)

    def add_others(i, j):
        for q in range(1, cores):
            for k in range(depth):
                arrived((group(i, j), member(k, q)))
            add(i, j, q)

    for k in range(1, depth):
        send((g, d), (g, member(depth - k, 0)), True)
    spread(0, True)

    row_hit = lax.broadcasted_iota(jnp.int32, (columns, slots), 0).astype(jnp.float32) == row
    col_hit = lax.broadcasted_iota(jnp.int32, (blocks_wide, slots), 0).astype(jnp.float32) == col
    taken = lax.dot_general(
        jnp.where(row_hit & used, 1.0, 0.0).astype(jnp.bfloat16),
        jnp.where(col_hit, 1.0, 0.0).astype(jnp.bfloat16),
        (((1,), (1,)), ((), ())),
        preferred_element_type=jnp.float32,
    )

    def keep(first, last):
        for c in range(first, last):
            kept[0, :, pl.ds(c * LANES, LANES)] = jnp.where(
                taken[:, c : c + 1] > 0.5, 0.0, summed[c]
            )

    order = sorted(range(1, depth), key=lambda k: min(k, depth - k))
    hops = [(k, i, j) for k in range(depth) for i, j in (
        [(0, j) for j in range(1, rows_b)] if k % 2 == 0 else [(i, 0) for i in range(1, rows_a)]
    )]

    def relay(k, i, j):
        slot = (group(i, j), member(k, 0))
        arrived(slot)
        if j:
            for n in range(1, rows_a):
                send(slot, (group(n, 0), d))
        else:
            for n in range(1, rows_b):
                send(slot, (group(0, n), d))
        to_partner(slot)

    for n, k in enumerate(order):
        keep(blocks_wide * n // len(order), blocks_wide * (n + 1) // len(order))
        arrived((g, member(k, 0)))
        spread(k)
    for k, i, j in hops:
        if k == 0:
            relay(k, i, j)
    add(0, 0, 0)
    for k, i, j in hops:
        if k:
            relay(k, i, j)
    add_others(0, 0)
    for i in range(rows_a):
        for j in range(rows_b):
            if i == 0 and j == 0:
                continue
            for k in range(depth):
                relayed = (k, i, j) in hops
                if not relayed:
                    slot = (group(i, j), member(k, 0))
                    arrived(slot)
                    to_partner(slot)
            add(i, j, 0)
            add_others(i, j)

    small[2].wait()
    for c in range(part_blocks):
        rows = pl.ds(c * columns, columns)
        cols = pl.ds(c * LANES, LANES)
        momentum_out[:, cols] = momentum_decay * momentum_in[:, cols] + (
            total[rows, pl.ds(0, LANES)] + total[rows, pl.ds(LANES, LANES)]
        )
    for copy in sends:
        copy.wait_send()


def finish_kernel(kept_in, momentum_in, kept, momentum, sem):
    copies = (
        pltpu.make_async_copy(momentum_in, momentum, sem.at[0]),
        pltpu.make_async_copy(kept_in, kept, sem.at[1]),
    )
    for copy in copies:
        copy.start()
    for copy in copies:
        copy.wait()


def local(mesh_sizes, acts, grads_out, residual_in, sel_index, sel_count, momentum_in):
    groups, members = mesh_sizes
    tokens, width = acts.shape
    columns = grads_out.shape[1]
    slots = sel_index.shape[1]
    part_width = momentum_in.shape[1]
    tiles = tiles_of(width)
    vmem = pl.BlockSpec(memory_space=pltpu.VMEM)
    smem = pl.BlockSpec(memory_space=pltpu.SMEM)
    hbm = pl.BlockSpec(memory_space=pltpu.HBM)
    rows_b = max(n for n in range(1, groups + 1) if groups % n == 0 and n * n <= groups)
    cores = 2 if members % 2 == 0 else 1
    rows_a, depth = groups // rows_b, members // cores
    sizes = (rows_a, rows_b, depth, cores)
    n_sends = depth - 1 + depth * (groups - 1) + depth * groups * (cores - 1)
    kept, momentum_out = pl.pallas_call(
        functools.partial(gather_kernel, tiles, sizes),
        out_shape=(
            pltpu.VMEM(residual_in.shape, jnp.float32),
            pltpu.VMEM(momentum_in.shape, jnp.float32),
        ),
        in_specs=[hbm, hbm, hbm, hbm, smem, smem, hbm],
        out_specs=(vmem, vmem),
        scratch_shapes=[
            pltpu.VMEM((columns, tokens), jnp.bfloat16),
            pltpu.VMEM((1, slots), jnp.int32),
            pltpu.VMEM(momentum_in.shape, jnp.float32),
            pltpu.SemaphoreType.DMA((3,)),
            pltpu.VMEM((tokens, width), jnp.bfloat16),
            pltpu.VMEM((columns, width), jnp.float32),
            pltpu.VMEM((width // LANES, columns, LANES), jnp.float32),
            pltpu.VMEM((slots + 8, LANES), jnp.float32),
            pltpu.VMEM((groups, members, slots + 8, LANES), jnp.float32),
            pltpu.VMEM((columns * part_width // LANES, 2 * LANES), jnp.float32),
            pltpu.SemaphoreType.DMA((2, tiles)),
            pltpu.SemaphoreType.DMA((n_sends,)),
            pltpu.SemaphoreType.DMA((groups, members)),
        ],
        compiler_params=pltpu.CompilerParams(
            collective_id=0, has_side_effects=True, vmem_limit_bytes=40 << 20
        ),
        name="gather",
    )(acts, residual_in, grads_out.T, sel_index, sel_index, sel_count, momentum_in)
    return pl.pallas_call(
        finish_kernel,
        out_shape=(
            jax.ShapeDtypeStruct(residual_in.shape, jnp.float32),
            jax.ShapeDtypeStruct(momentum_in.shape, jnp.float32),
        ),
        in_specs=[vmem, vmem],
        out_specs=(hbm, hbm),
        scratch_shapes=[pltpu.SemaphoreType.DMA((2,))],
        compiler_params=pltpu.CompilerParams(vmem_limit_bytes=8 << 20),
        name="finish",
    )(kept, momentum_out)


def solution(mesh):
    placed = (
        P(("grp", "dev"), None),
        P(("grp", "dev"), None),
        P(("grp", "dev"), None, None),
        P(("grp", "dev"), None),
        P(("grp", "dev")),
        P(None, "dev"),
    )
    return jax.shard_map(
        functools.partial(local, (mesh.shape["grp"], mesh.shape["dev"])),
        mesh=mesh,
        in_specs=placed,
        out_specs=(P(("grp", "dev"), None, None), P(None, "dev")),
        check_vma=False,
    )
```

```python
import functools

import jax
import jax.numpy as jnp
from jax import lax
from jax.experimental import pallas as pl
from jax.experimental.pallas import tpu as pltpu
from jax.sharding import PartitionSpec as P

momentum_decay = 0.9
LANES = 128
vmem_bytes = 67043328
MESH = pl.DeviceIdType.MESH


def tiles_of(width):
    for count in (8, 6, 4, 3, 2):
        if width % (count * 2 * LANES) == 0:
            return count
    return 1


def gather_kernel(
    tiles, sizes, acts, residual, grads_in, sel_in, sel_smem, count_smem, momentum_hbm,
    kept, momentum_out,
    grads, sel_row, momentum_in, small_sem, acts_buf, res_buf, summed, packed, store, total, in_sem, send_sem, recv_sem,
):
    columns, width = residual.shape[1:]
    slots = sel_row.shape[1]
    blocks_wide = width // LANES
    span = width // tiles
    per_tile = span // LANES

    def fetch(t):
        cols = pl.ds(t * span, span)
        return (
            pltpu.make_async_copy(acts.at[:, cols], acts_buf.at[:, cols], in_sem.at[0, t]),
            pltpu.make_async_copy(residual.at[0, :, cols], res_buf.at[:, cols], in_sem.at[1, t]),
        )

    small = [
        pltpu.make_async_copy(sel_in, sel_row, small_sem.at[0]),
        pltpu.make_async_copy(grads_in, grads, small_sem.at[1]),
        pltpu.make_async_copy(momentum_hbm, momentum_in, small_sem.at[2]),
    ]
    for copy in small[:2]:
        copy.start()
    for t in range(tiles):
        for copy in fetch(t):
            copy.start()
    small[2].start()

    rows_a, rows_b, depth, cores = sizes
    part_width = momentum_in.shape[1]
    part_blocks = part_width // LANES
    g = lax.axis_index("grp")
    d = lax.axis_index("dev")
    a, b = g // rows_b, g % rows_b
    z, core = d // cores, d % cores

    def group(i, j):
        return lax.rem(a + i, rows_a) * rows_b + lax.rem(b + j, rows_b)

    near = [sorted(range(depth), key=lambda y: (abs(y - x), y)) for x in range(depth)]

    def member(k, q):
        place = near[0][k]
        for x in range(1, depth):
            place = jnp.where(z == x, near[x][k], place)
        return place * cores + lax.rem(core + q, cores)

    peers = (
        [(g, member(k, 0)) for k in range(1, depth)]
        + [(g, member(0, q)) for q in range(1, cores)]
        + [(group(i, 0), d) for i in range(1, rows_a)]
        + [(group(0, j), d) for j in range(1, rows_b)]
        + [(group(i, j), d) for i in range(1, rows_a) for j in range(1, rows_b) if 0 < depth]
    )
    barrier = pltpu.get_barrier_semaphore()
    for peer in peers:
        pl.semaphore_signal(barrier, inc=1, device_id=peer, device_id_type=MESH)

    small[0].wait()
    number = sel_row[...].astype(jnp.float32)
    row = jnp.floor((number + 0.5) * (1.0 / blocks_wide))
    col = number - row * blocks_wide
    used = lax.broadcasted_iota(jnp.int32, (1, slots), 1) < count_smem[0]
    label = jnp.where(used, col * columns + row, -1.0)
    packed[pl.ds(slots, 8), pl.ds(0, slots)] = jnp.broadcast_to(label, (8, slots))
    if slots < LANES:
        packed[pl.ds(slots, 8), pl.ds(slots, LANES - slots)] = jnp.full(
            (8, LANES - slots), -1.0, jnp.float32
        )

    small[1].wait()
    turned = grads[...]
    for t in range(tiles):
        for copy in fetch(t):
            copy.wait()
        cols = pl.ds(t * span, span)
        sums = res_buf[:, cols] + jnp.dot(
            turned, acts_buf[:, cols], preferred_element_type=jnp.float32
        )
        for j in range(per_tile):
            summed[t * per_tile + j] = sums[:, j * LANES : (j + 1) * LANES]
    for s in range(slots):
        block = sel_smem[0, s]
        r = lax.div(block, blocks_wide)
        packed[pl.ds(s, 1), :] = summed[block - r * blocks_wide, pl.ds(r, 1), :]
    store[g, d] = packed[...]
    pl.semaphore_wait(barrier, len(peers))

    sends = []

    def copy_to(source, slot, peer, index):
        return pltpu.make_async_remote_copy(
            src_ref=source,
            dst_ref=store.at[slot[0], slot[1]],
            send_sem=send_sem.at[index],
            recv_sem=recv_sem.at[slot[0], slot[1]],
            device_id=peer,
            device_id_type=MESH,
        )

    def send(slot, peer, own=False):
        source = packed if own else store.at[slot[0], slot[1]]
        copy = copy_to(source, slot, peer, len(sends))
        sends.append(copy)
        copy.start()

    def arrived(slot):
        copy_to(store.at[slot[0], slot[1]], slot, (g, member(0, 1)), 0).wait_recv()

    def to_partner(slot, own=False):
        for q in range(1, cores):
            send(slot, (g, member(0, q)), own)

    def spread(k, own=False):
        slot = (g, member(k, 0))
        for i in range(1, rows_a):
            send(slot, (group(i, 0), d), own)
        for j in range(1, rows_b):
            send(slot, (group(0, j), d), own)
        if k >= 0:
            for i in range(1, rows_a):
                for j in range(1, rows_b):
                    send(slot, (group(i, j), d), own)
        to_partner(slot, own)

    base = (d * (part_blocks * columns)).astype(jnp.float32)
    place = lax.broadcasted_iota(jnp.int32, (part_blocks * columns, 1), 0).astype(jnp.float32)
    started = []

    def add(i, j, q):
        blocks = [(group(i, j), member(k, q)) for k in range(depth)]
        vals = jnp.concatenate([store[x, y, :slots, :] for x, y in blocks], axis=0)
        labels = jnp.concatenate(
            [store[x, y, pl.ds(slots, 1), pl.ds(0, slots)] for x, y in blocks], axis=1
        )
        high = vals.astype(jnp.bfloat16)
        low = (vals - high.astype(jnp.float32)).astype(jnp.bfloat16)
        both = jnp.concatenate([high, low], axis=1)
        hit = jnp.where(place == labels - base, 1.0, 0.0).astype(jnp.bfloat16)
        part = jnp.dot(hit, both, preferred_element_type=jnp.float32)
        if started:
            total[...] += part
        else:
            total[...] = part
            started.append(True)

    def add_others(i, j):
        for q in range(1, cores):
            for k in range(depth):
                arrived((group(i, j), member(k, q)))
            add(i, j, q)

    for k in range(depth - 1, 0, -1):
        send((g, d), (g, member(k, 0)), True)
    spread(0, True)

    row_hit = lax.broadcasted_iota(jnp.int32, (columns, slots), 0).astype(jnp.float32) == row
    col_hit = lax.broadcasted_iota(jnp.int32, (blocks_wide, slots), 0).astype(jnp.float32) == col
    taken = lax.dot_general(
        jnp.where(row_hit & used, 1.0, 0.0).astype(jnp.bfloat16),
        jnp.where(col_hit, 1.0, 0.0).astype(jnp.bfloat16),
        (((1,), (1,)), ((), ())),
        preferred_element_type=jnp.float32,
    )

    def keep(first, last):
        for c in range(first, last):
            kept[0, :, pl.ds(c * LANES, LANES)] = jnp.where(
                taken[:, c : c + 1] > 0.5, 0.0, summed[c]
            )

    def relayed(k):
        if k % 2 == 0:
            return [(0, j) for j in range(1, rows_b)]
        return [(i, 0) for i in range(1, rows_a)]

    def straight(k):
        if k % 2 == 0:
            return [(i, 0) for i in range(1, rows_a)]
        return [(0, j) for j in range(1, rows_b)]

    def pass_on(k):
        for i, j in relayed(k):
            slot = (group(i, j), member(k, 0))
            arrived(slot)
            if k < 0:
                if j:
                    for n in range(1, rows_a):
                        send(slot, (group(n, 0), d))
                else:
                    for n in range(1, rows_b):
                        send(slot, (group(0, n), d))
            to_partner(slot)
        for i, j in straight(k):
            slot = (group(i, j), member(k, 0))
            arrived(slot)
            to_partner(slot)

    def pass_far(k):
        for i in range(1, rows_a):
            for j in range(1, rows_b):
                slot = (group(i, j), member(k, 0))
                arrived(slot)
                to_partner(slot)

    for k in range(1, depth):
        keep(blocks_wide * (k - 1) // (depth - 1), blocks_wide * k // (depth - 1))
        arrived((g, member(k, 0)))
        spread(k)
        pass_on(k - 1)
    add(0, 0, 0)
    for k in range(depth - 1):
        pass_far(k)
    pass_on(depth - 1)
    add_others(0, 0)
    for i in range(rows_a):
        for j in range(rows_b):
            if (i == 0) != (j == 0):
                add(i, j, 0)
    pass_far(depth - 1)
    for i in range(rows_a):
        for j in range(rows_b):
            if i and j:
                add(i, j, 0)
    for i in range(rows_a):
        for j in range(rows_b):
            if i or j:
                add_others(i, j)

    small[2].wait()
    for c in range(part_blocks):
        rows = pl.ds(c * columns, columns)
        cols = pl.ds(c * LANES, LANES)
        momentum_out[:, cols] = momentum_decay * momentum_in[:, cols] + (
            total[rows, pl.ds(0, LANES)] + total[rows, pl.ds(LANES, LANES)]
        )
    for copy in sends:
        copy.wait_send()


def finish_kernel(kept_in, momentum_in, kept, momentum, sem):
    copies = (
        pltpu.make_async_copy(momentum_in, momentum, sem.at[0]),
        pltpu.make_async_copy(kept_in, kept, sem.at[1]),
    )
    for copy in copies:
        copy.start()
    for copy in copies:
        copy.wait()


def local(mesh_sizes, acts, grads_out, residual_in, sel_index, sel_count, momentum_in):
    groups, members = mesh_sizes
    tokens, width = acts.shape
    columns = grads_out.shape[1]
    slots = sel_index.shape[1]
    part_width = momentum_in.shape[1]
    tiles = tiles_of(width)
    vmem = pl.BlockSpec(memory_space=pltpu.VMEM)
    smem = pl.BlockSpec(memory_space=pltpu.SMEM)
    hbm = pl.BlockSpec(memory_space=pltpu.HBM)
    rows_b = max(n for n in range(1, groups + 1) if groups % n == 0 and n * n <= groups)
    cores = 2 if members % 2 == 0 else 1
    rows_a, depth = groups // rows_b, members // cores
    sizes = (rows_a, rows_b, depth, cores)
    n_sends = depth - 1 + depth * (groups - 1) + depth * groups * (cores - 1)
    results = 4 * (columns * width + columns * part_width)
    room = (vmem_bytes - results - (16 << 10)) // 4096 * 4096
    kept, momentum_out = pl.pallas_call(
        functools.partial(gather_kernel, tiles, sizes),
        out_shape=(
            pltpu.VMEM(residual_in.shape, jnp.float32),
            pltpu.VMEM(momentum_in.shape, jnp.float32),
        ),
        in_specs=[hbm, hbm, hbm, hbm, smem, smem, hbm],
        out_specs=(vmem, vmem),
        scratch_shapes=[
            pltpu.VMEM((columns, tokens), jnp.bfloat16),
            pltpu.VMEM((1, slots), jnp.int32),
            pltpu.VMEM(momentum_in.shape, jnp.float32),
            pltpu.SemaphoreType.DMA((3,)),
            pltpu.VMEM((tokens, width), jnp.bfloat16),
            pltpu.VMEM((columns, width), jnp.float32),
            pltpu.VMEM((width // LANES, columns, LANES), jnp.float32),
            pltpu.VMEM((slots + 8, LANES), jnp.float32),
            pltpu.VMEM((groups, members, slots + 8, LANES), jnp.float32),
            pltpu.VMEM((columns * part_width // LANES, 2 * LANES), jnp.float32),
            pltpu.SemaphoreType.DMA((2, tiles)),
            pltpu.SemaphoreType.DMA((n_sends,)),
            pltpu.SemaphoreType.DMA((groups, members)),
        ],
        compiler_params=pltpu.CompilerParams(
            collective_id=0, has_side_effects=True, vmem_limit_bytes=room
        ),
        name="gather",
    )(acts, residual_in, grads_out.T, sel_index, sel_index, sel_count, momentum_in)
    return pl.pallas_call(
        finish_kernel,
        out_shape=(
            jax.ShapeDtypeStruct(residual_in.shape, jnp.float32),
            jax.ShapeDtypeStruct(momentum_in.shape, jnp.float32),
        ),
        in_specs=[vmem, vmem],
        out_specs=(hbm, hbm),
        scratch_shapes=[pltpu.SemaphoreType.DMA((2,))],
        compiler_params=pltpu.CompilerParams(vmem_limit_bytes=8 << 20),
        name="finish",
    )(kept, momentum_out)


def solution(mesh):
    placed = (
        P(("grp", "dev"), None),
        P(("grp", "dev"), None),
        P(("grp", "dev"), None, None),
        P(("grp", "dev"), None),
        P(("grp", "dev")),
        P(None, "dev"),
    )
    return jax.shard_map(
        functools.partial(local, (mesh.shape["grp"], mesh.shape["dev"])),
        mesh=mesh,
        in_specs=placed,
        out_specs=(P(("grp", "dev"), None, None), P(None, "dev")),
        check_vma=False,
    )
```
